32 devices in a mesh: row: 8 (over y, x, core), col: 4 (over z).
Axes of the slice: x: 2, y: 2, z: 4, core: 2. Of those that a mesh axis runs over, the one named last changes fastest.
Arguments:
- tokens: bfloat16 [1024, 8192], P('row', 'col'), may hold values from -6 to 6
- weights: bfloat16 [2, 14336, 8192], P(None, 'row', 'col'), may hold values from -0.0625 to 0.0625
- gradients: bfloat16 [2, 14336, 8192], P(None, 'row', 'col'), may hold values from -200 to 200, as said below
- row_factors: float32 [2, 14336], P(None, 'row'), may hold values from 0.05 to 0.5
- col_factors: float32 [2, 8192], P(None, 'col'), may hold values from 0.05 to 0.5
Outputs:
- hidden: bfloat16 [1024, 14336], P('col', 'row')
- row_new: float32 [2, 14336], P(None, 'row')
- col_new: float32 [2, 8192], P(None, 'col')
The draws below stay inside these ranges and needn't reach their ends.
Inputs may be any that keep to these rules, and one draw needn't show every extreme that they name: Finite real gradients.
All inputs are finite; a program needn't handle non-finite values.
Results may differ from the reference program's by a relative error of at most 0.001.
The reference program's roundings to bfloat16 on the way (of `new_weights`) count: a program that leaves them out, or rounds other values in their place, can miss the bound.
Values may be sent and summed in bfloat16 or wider, within the bound.
No kernel may reach another device: no remote copies, remote signals or barrier semaphores. Data moves between devices by JAX's collectives and lax.ppermute only.
A program may use at most 128 MiB of HBM per device.

```python
import math
import jax
import jax.numpy as jnp
from jax import lax

D = 8192
FF = 14336
TOKENS = 1024


def draw_gradients(key, part):
    keys = jax.random.split(jax.random.fold_in(key, 17), 5)
    row_pos = jnp.arange(FF, dtype=jnp.float32) / FF
    col_pos = jnp.arange(D, dtype=jnp.float32) / D
    row_scale = 0.5 * jnp.power(3.0, row_pos)[None, :, None] * jnp.exp(jax.random.uniform(keys[0], (2, FF, 1), jnp.float32, math.log(0.4), math.log(2.5)))
    col_scale = 0.5 * jnp.power(3.0, col_pos)[None, None, :] * jnp.exp(jax.random.uniform(keys[1], (2, 1, D), jnp.float32, math.log(0.4), math.log(2.5)))
    values = jax.random.normal(keys[4], (2, FF, D), jnp.float32) * row_scale * col_scale
    return jnp.clip(values, -200.0, 200.0).astype(jnp.bfloat16)


def block_levels(key, dims, shards, least, largest):
    gain = 1.0
    for dim, parts in shards:
        heights = jax.random.uniform(jax.random.fold_in(jax.random.fold_in(key, 6), dim), (parts,), jnp.float32, least / len(shards), largest / len(shards))
        gain = gain * jnp.repeat(jnp.exp(heights), dims[dim] // parts).reshape((-1,) + (1,) * (len(dims) - 1 - dim))
    return gain


def bell_draw(rng, shape, deviation, limit, cuts=(), kind=jnp.bfloat16):
    gain = block_levels(rng, shape, cuts, -0.22, 0.18) if cuts else 1.0
    values = jax.random.normal(rng, shape, jnp.float32) * deviation * gain
    return jnp.minimum(jnp.maximum(values, -limit), limit).astype(kind)


def setup_inputs(seed: int = 0) -> dict:
    key_list = jax.random.split(jax.random.key(seed), 6)
    return {
        "tokens": bell_draw(key_list[0], (TOKENS, D), 1.0, 6.0, ((0, 8), (1, 4))),
        "weights": bell_draw(key_list[1], (2, FF, D), D ** -0.5, 0.0625, ((1, 8), (2, 4))),
        "gradients": draw_gradients(jax.random.fold_in(key_list[5], 71), 0),
        "row_factors": jnp.clip(jnp.exp(math.log(0.5) - 2.3025851 * jax.random.uniform(key_list[3], (2, FF), jnp.float32) ** block_levels(key_list[3], (2, FF), ((1, 8),), -0.2, 0.2)), 0.05, 0.5),
        "col_factors": jnp.clip(jnp.exp(math.log(0.5) - 2.3025851 * jax.random.uniform(key_list[4], (2, D), jnp.float32) ** block_levels(key_list[4], (2, D), ((1, 4),), -0.2, 0.2)), 0.05, 0.5),
    }


decay_rate = 0.5
learn_rate = 0.01
clip_limit = 1.0
tiny_eps = 1e-30

def reference(tokens, weights, gradients, row_factors, col_factors):
    gradient = gradients.astype(jnp.float32)
    squares = gradient * gradient
    row_new = decay_rate * row_factors + (1.0 - decay_rate) * (lax.optimization_barrier(jnp.mean(squares, axis=2)) + tiny_eps)
    col_new = decay_rate * col_factors + (1.0 - decay_rate) * (lax.optimization_barrier(jnp.mean(squares, axis=1)) + tiny_eps)
    row_mean = lax.optimization_barrier(jnp.mean(row_new, axis=1))
    denominator = jnp.sqrt(row_new[:, :, None] * col_new[:, None, :] / row_mean[:, None, None])
    update = gradient / denominator
    rms_value = jnp.sqrt(lax.optimization_barrier(jnp.mean(update * update, axis=(1, 2))))
    clip_scale = jnp.maximum(1.0, rms_value / clip_limit)
    new_weights = (weights.astype(jnp.float32) - learn_rate * update / clip_scale[:, None, None]).astype(jnp.bfloat16)
    gate_proj = lax.dot_general(tokens, new_weights[0], (((1,), (1,)), ((), ())), preferred_element_type=jnp.float32)
    up_proj = lax.dot_general(tokens, new_weights[1], (((1,), (1,)), ((), ())), preferred_element_type=jnp.float32)
    hidden = (jax.nn.silu(gate_proj) * up_proj).astype(jnp.bfloat16)
    return (hidden, row_new, col_new)
```

```python
import jax
import jax.numpy as jnp
from jax import lax
from jax.sharding import PartitionSpec as P

decay_rate = 0.5
learn_rate = 0.01
clip_limit = 1.0
tiny_eps = 1e-30

OWN_GATHER = True
OWN_SUM = True
PIECES = 2


def swap(x, axis, size, bit):
    return lax.ppermute(x, axis, [(k, k ^ bit) for k in range(size)])


def total(x, axis, size):
    if size & (size - 1) or not OWN_SUM:
        return lax.psum(x, axis)
    bit = 1
    while bit < size:
        x = x + swap(x, axis, size, bit)
        bit *= 2
    return x


def gather(x, axis, size):
    if size & (size - 1) or not OWN_GATHER:
        return lax.all_gather(x, axis, axis=0, tiled=True)
    place = lax.axis_index(axis)
    rows, width = x.shape
    blocks = x.reshape((1,) * (size.bit_length() - 1) + x.shape)
    for level in range(size.bit_length() - 1):
        bit = size >> (level + 1)
        other = swap(blocks, axis, size, bit)
        low = (place & bit) == 0
        blocks = jnp.concatenate(
            [jnp.where(low, blocks, other), jnp.where(low, other, blocks)], axis=level
        )
    return blocks.reshape(size * rows, width)


def make(n_row, n_col):
    def local(tokens, weights, gradients, row_factors, col_factors):
        row_block, col_block = gradients.shape[1:]
        n_hidden = row_block * n_row
        n_feature = col_block * n_col
        spread = gather(tokens, "row", n_row)
        gradient = gradients.astype(jnp.float32)
        squares = gradient * gradient
        row_total = total(jnp.sum(squares, axis=2), "col", n_col)
        col_total = total(jnp.sum(squares, axis=1), "row", n_row)
        row_new = decay_rate * row_factors + (1.0 - decay_rate) * (row_total / n_feature + tiny_eps)
        col_new = decay_rate * col_factors + (1.0 - decay_rate) * (col_total / n_hidden + tiny_eps)
        row_inv = 1.0 / row_new
        col_inv = 1.0 / col_new
        norm_part = jnp.sum(
            jnp.sum(gradient * gradient * col_inv[:, None, :], axis=2) * row_inv, axis=1
        )
        both = jnp.stack([norm_part, jnp.sum(row_new, axis=1) / n_col])
        both = total(total(both, "col", n_col), "row", n_row)
        row_mean = both[1] / n_hidden
        rms = jnp.sqrt(both[0] * row_mean / (n_hidden * n_feature))
        clip_scale = jnp.maximum(1.0, rms / clip_limit)
        row_gain = jnp.sqrt(row_mean[:, None] * row_inv) * (learn_rate / clip_scale)[:, None]
        col_gain = jnp.sqrt(col_inv)

        place = lax.axis_index("col")
        block = spread.shape[0] // n_col
        size = row_block // PIECES
        tok = [
            lax.dynamic_slice_in_dim(spread, ((place + k) % n_col) * block, block, axis=0)
            for k in range(n_col)
        ]

        def piece(h, q):
            cut = slice(q * size, (q + 1) * size)
            new = (
                weights[h, cut].astype(jnp.float32)
                - gradients[h, cut].astype(jnp.float32)
                * (row_gain[h, cut][:, None] * col_gain[h][None, :])
            ).astype(jnp.bfloat16)
            step = 1 if h == 0 else -1
            ring = [(k, (k + step) % n_col) for k in range(n_col)]

            def part(s):
                value = lax.dot_general(
                    tok[(-step * (1 + s)) % n_col], new, (((1,), (1,)), ((), ())),
                    preferred_element_type=jnp.float32,
                )
                return lax.optimization_barrier(value)

            acc = part(0)
            for s in range(1, n_col):
                acc = lax.ppermute(acc, "col", ring) + part(s)
            return acc

        outs = []
        for q in range(PIECES):
            gate_proj = piece(0, q)
            up_proj = piece(1, q)
            outs.append((jax.nn.silu(gate_proj) * up_proj).astype(jnp.bfloat16))
        hidden = jnp.concatenate(outs, axis=1)
        return (hidden, row_new, col_new)

    return local


def solution(mesh):
    placed = (
        P("row", "col"),
        P(None, "row", "col"),
        P(None, "row", "col"),
        P(None, "row"),
        P(None, "col"),
    )
    return jax.shard_map(
        make(mesh.shape["row"], mesh.shape["col"]),
        mesh=mesh,
        in_specs=placed,
        out_specs=(P("col", "row"), P(None, "row"), P(None, "col")),
        check_vma=False,
    )
```

```python
import jax
import jax.numpy as jnp
from jax import lax
from jax.sharding import PartitionSpec as P

decay_rate = 0.5
learn_rate = 0.01
clip_limit = 1.0
tiny_eps = 1e-30

OWN_GATHER = True
OWN_SUM = True
PIECES = 2


def swap(x, axis, size, bit):
    return lax.ppermute(x, axis, [(k, k ^ bit) for k in range(size)])


def total(x, axis, size):
    if size & (size - 1) or not OWN_SUM:
        return lax.psum(x, axis)
    bit = 1
    while bit < size:
        x = x + swap(x, axis, size, bit)
        bit *= 2
    return x


def gather(x, axis, size):
    if size & (size - 1) or not OWN_GATHER:
        return lax.all_gather(x, axis, axis=0, tiled=True)
    place = lax.axis_index(axis)
    rows, width = x.shape
    blocks = x.reshape((1,) * (size.bit_length() - 1) + x.shape)
    for level in range(size.bit_length() - 1):
        bit = size >> (level + 1)
        other = swap(blocks, axis, size, bit)
        low = (place & bit) == 0
        blocks = jnp.concatenate(
            [jnp.where(low, blocks, other), jnp.where(low, other, blocks)], axis=level
        )
    return blocks.reshape(size * rows, width)


def make(n_row, n_col):
    def local(tokens, weights, gradients, row_factors, col_factors):
        row_block, col_block = gradients.shape[1:]
        n_hidden = row_block * n_row
        n_feature = col_block * n_col
        spread = gather(tokens, "row", n_row)
        gradient = gradients.astype(jnp.float32)
        squares = gradient * gradient
        row_total = total(jnp.sum(squares, axis=2), "col", n_col)
        col_total = total(jnp.sum(squares, axis=1), "row", n_row)
        row_new = decay_rate * row_factors + (1.0 - decay_rate) * (row_total / n_feature + tiny_eps)
        col_new = decay_rate * col_factors + (1.0 - decay_rate) * (col_total / n_hidden + tiny_eps)
        row_inv = 1.0 / row_new
        col_inv = 1.0 / col_new
        norm_part = jnp.sum(
            jnp.sum(gradient * gradient * col_inv[:, None, :], axis=2) * row_inv, axis=1
        )
        both = jnp.stack([norm_part, jnp.sum(row_new, axis=1) / n_col])
        both = total(total(both, "col", n_col), "row", n_row)
        row_mean = both[1] / n_hidden
        rms = jnp.sqrt(both[0] * row_mean / (n_hidden * n_feature))
        clip_scale = jnp.maximum(1.0, rms / clip_limit)
        row_gain = jnp.sqrt(row_mean[:, None] * row_inv) * (learn_rate / clip_scale)[:, None]
        col_gain = jnp.sqrt(col_inv)

        place = lax.axis_index("col")
        block = spread.shape[0] // n_col
        size = row_block // PIECES
        tok = [
            lax.dynamic_slice_in_dim(spread, ((place + k) % n_col) * block, block, axis=0)
            for k in range(n_col)
        ]

        def piece(h, q, gain):
            cut = slice(q * size, (q + 1) * size)
            new = (
                weights[h, cut].astype(jnp.float32)
                - gradients[h, cut].astype(jnp.float32)
                * (gain[h, cut][:, None] * col_gain[h][None, :])
            ).astype(jnp.bfloat16)
            step = 1 if h == 0 else -1
            ring = [(k, (k + step) % n_col) for k in range(n_col)]

            def part(s):
                value = lax.dot_general(
                    tok[(-step * (1 + s)) % n_col], new, (((1,), (1,)), ((), ())),
                    preferred_element_type=jnp.float32,
                )
                return lax.optimization_barrier(value)

            return part, ring

        def go_round(part, ring, acc):
            for s in range(1, n_col):
                acc = lax.ppermute(acc, "col", ring) + part(s)
            return acc

        outs = []
        for q in range(PIECES):
            gate = piece(0, q, row_gain)
            up = piece(1, q, row_gain)
            row_gain, first_gate, first_up = lax.optimization_barrier(
                (row_gain, gate[0](0), up[0](0))
            )
            gate_proj = go_round(*gate, first_gate)
            up_proj = go_round(*up, first_up)
            outs.append((jax.nn.silu(gate_proj) * up_proj).astype(jnp.bfloat16))
        hidden = jnp.concatenate(outs, axis=1)
        return (hidden, row_new, col_new)

    return local


def solution(mesh):
    placed = (
        P("row", "col"),
        P(None, "row", "col"),
        P(None, "row", "col"),
        P(None, "row"),
        P(None, "col"),
    )
    return jax.shard_map(
        make(mesh.shape["row"], mesh.shape["col"]),
        mesh=mesh,
        in_specs=placed,
        out_specs=(P("col", "row"), P(None, "row"), P(None, "col")),
        check_vma=False,
    )
```
